32 devices in a mesh: dp: 1 (over z), tp: 4 (over y), ep: 8 (over x, core).
Axes of the slice: x: 4, y: 4, z: 1, core: 2. Of those that a mesh axis runs over, the one named last changes fastest.
The devices are a block of a 4x4x8 slice.
Arguments:
- tokens: bfloat16 [8192, 768], P(('dp', 'ep', 'tp'))
- expert_ids: int32 [8192, 2], P(('dp', 'ep', 'tp'))
- gate_vals: float32 [8192, 2], P(('dp', 'ep', 'tp'))
- w_up: bfloat16 [64, 768, 3072], P('ep', None, 'tp')
- w_down: bfloat16 [64, 3072, 768], P('ep', 'tp')
Outputs:
- output: bfloat16 [8192, 768], P(('dp', 'ep', 'tp'))
All inputs are finite; a program needn't handle non-finite values.
Results may differ from the reference program's by a relative error of at most 0.001.
Values are sent between devices in bfloat16 or wider.
A program may use at most 768 MiB of HBM per device.

```python
import jax
import jax.numpy as jnp
from jax import lax

EXPERTS = 64
TOP_K = 2
HIDDEN = 768
FFN_DIM = 3072
TOK_DEV = 256
EP_SIZE = 8
TP_SIZE = 4

N_SOURCES = EP_SIZE * TP_SIZE
SLOT_CAP = ((5 * TOK_DEV * TOP_K) // (4 * EXPERTS) + 7) // 8 * 8
N_SLOTS = EXPERTS * SLOT_CAP
N_HOT = max(1, EXPERTS // (8 * TOP_K))
HOT_FILL = SLOT_CAP + SLOT_CAP // 8


def draw_routes(perm_key, order_key, offset_key):
    hot_perm = jax.random.permutation(perm_key, EXPERTS).astype(jnp.int32)
    ranks = jnp.arange(TOK_DEV, dtype=jnp.int32)
    first_rank = jnp.where(ranks < N_HOT * HOT_FILL, ranks // HOT_FILL,
                           N_HOT + (ranks - N_HOT * HOT_FILL) % (EXPERTS - N_HOT))
    orders = jax.vmap(lambda sub_key: jax.random.permutation(sub_key, TOK_DEV))(
        jax.random.split(order_key, N_SOURCES))
    first_choice = hot_perm[first_rank[orders]]
    scores = jax.random.randint(offset_key, (N_SOURCES, TOK_DEV, EXPERTS - 1), 0, 2 ** 20) * (EXPERTS - 1)
    scores = scores + jnp.arange(EXPERTS - 1, dtype=jnp.int32)
    picked = lax.top_k(scores, TOP_K)[1][:, :, :TOP_K - 1] + 1
    others = (first_choice[:, :, None] + picked) % EXPERTS
    routes = jnp.concatenate([first_choice[:, :, None], others], axis=2)
    return routes.reshape(N_SOURCES * TOK_DEV, TOP_K).astype(jnp.int32)


def setup_inputs(seed: int = 0, part: int = 0) -> dict:
    part_keys = jax.random.split(jax.random.fold_in(jax.random.key(seed), part), 5)
    weight_keys = jax.random.split(jax.random.key(seed + 1), 2)
    tokens = jax.random.normal(part_keys[0], (N_SOURCES * TOK_DEV, HIDDEN), jnp.float32).astype(jnp.bfloat16)
    expert_ids = draw_routes(part_keys[1], part_keys[2], part_keys[3])
    gate_vals = jax.random.uniform(part_keys[4], (N_SOURCES * TOK_DEV, TOP_K), jnp.float32, 0.5, 1.0)
    w_up = (jax.random.normal(weight_keys[0], (EXPERTS, HIDDEN, FFN_DIM), jnp.float32) * HIDDEN ** -0.5).astype(jnp.bfloat16)
    w_down = (jax.random.normal(weight_keys[1], (EXPERTS, FFN_DIM, HIDDEN), jnp.float32) * FFN_DIM ** -0.5).astype(jnp.bfloat16)
    return {'tokens': tokens, 'expert_ids': expert_ids, 'gate_vals': gate_vals, 'w_up': w_up, 'w_down': w_down}


def slot_table(route_ids):
    expert_hit = (route_ids[:, :, None] == jnp.arange(EXPERTS, dtype=jnp.int32)).astype(jnp.int32)
    chosen = jnp.sum(expert_hit, axis=1)
    prior_count = jnp.cumsum(chosen, axis=0) - chosen
    token_rank = jnp.sum(expert_hit * prior_count[:, None, :], axis=2)
    return jnp.where(token_rank < SLOT_CAP, route_ids * SLOT_CAP + token_rank, -1)


def reference(tokens, expert_ids, gate_vals, w_up, w_down):
    src_rows = tokens.reshape(N_SOURCES, TOK_DEV, HIDDEN)
    src_slots = jax.vmap(slot_table)(expert_ids.reshape(N_SOURCES, TOK_DEV, TOP_K))
    src_gates = gate_vals.reshape(N_SOURCES, TOK_DEV, TOP_K)
    slot_iota = jnp.arange(N_SLOTS, dtype=jnp.int32)

    def dispatch(operands):
        rows_in, slot_ids = operands
        pick_mat = jnp.zeros((N_SLOTS, TOK_DEV), jnp.bfloat16)
        for choice_idx in range(TOP_K):
            pick_mat = pick_mat + (slot_iota[:, None] == slot_ids[None, :, choice_idx]).astype(jnp.bfloat16)
        return jnp.dot(pick_mat, rows_in, preferred_element_type=jnp.float32).astype(jnp.bfloat16)

    buffers = lax.map(dispatch, (src_rows, src_slots))
    per_expert = jnp.transpose(buffers.reshape(N_SOURCES, EXPERTS, SLOT_CAP, HIDDEN), (1, 0, 2, 3))
    per_expert = per_expert.reshape(EXPERTS, N_SOURCES * SLOT_CAP, HIDDEN)

    def expert_ffn(operands):
        rows_in, up_mat, down_mat = operands
        pre_act = jnp.dot(rows_in, up_mat, preferred_element_type=jnp.float32)
        hidden_act = jax.nn.gelu(pre_act, approximate=True).astype(jnp.bfloat16)
        return jnp.dot(hidden_act, down_mat, preferred_element_type=jnp.float32).astype(jnp.bfloat16)

    expert_out = lax.map(expert_ffn, (per_expert, w_up, w_down))
    slot_out = jnp.transpose(expert_out.reshape(EXPERTS, N_SOURCES, SLOT_CAP, HIDDEN), (1, 0, 2, 3))
    slot_out = slot_out.reshape(N_SOURCES, N_SLOTS, HIDDEN)

    def combine(operands):
        results, slot_ids, gate_rows = operands
        gate_sum = jnp.zeros((TOK_DEV, HIDDEN), jnp.float32)
        for choice_idx in range(TOP_K):
            pick_mat = (slot_ids[:, choice_idx, None] == slot_iota[None, :]).astype(jnp.bfloat16)
            picked = jnp.dot(pick_mat, results, preferred_element_type=jnp.float32)
            gate_sum = gate_sum + gate_rows[:, choice_idx, None] * picked
        return gate_sum.astype(jnp.bfloat16)

    moe_out = lax.map(combine, (slot_out, src_slots, src_gates))
    return moe_out.reshape(N_SOURCES * TOK_DEV, HIDDEN)
```

```python
import functools

import jax
import jax.numpy as jnp
from jax import lax
from jax.experimental import pallas as pl
from jax.experimental.pallas import tpu as pltpu
from jax.sharding import PartitionSpec as P

MESH = pl.DeviceIdType.MESH
ID_ROWS = 16


def capacity(tok_count, n_top, n_exp):
    return ((5 * tok_count * n_top) // (4 * n_exp) + 7) // 8 * 8


def rem(a, b):
    return a % b if isinstance(a, int) else lax.rem(a, b)


def div(a, b):
    return a // b if isinstance(a, int) else lax.div(a, b)


def moe_kernel(n_tp, n_ep, slot_cap, tokens, id_rows, ids_col, gates, w_up, w_down, out,
               tok, up, down, tri, xbuf, part, r1, r2, red, ret, slot_col, acc,
               load_sem, w_sem, full_send, full_recv, half_send, half_recv,
               r1_send, r1_recv, r2_send, r2_recv, ret_send, ret_recv):
    t = lax.axis_index("tp")
    e = lax.axis_index("ep")
    n_chip = n_ep // 2
    x = div(e, 2)
    c = rem(e, 2)
    n_tok, hidden = tokens.shape
    n_loc = w_up.shape[0]
    n_top = ids_col.shape[1]
    n_exp = n_loc * n_ep
    rows = n_tok + ID_ROWS
    half_rows = n_tok // 2
    half_exp = n_loc // 2
    sub_rows = half_exp * slot_cap
    sub_half = sub_rows // 2
    n_sub = 2 * n_ep
    t_up = rem(t + 1, n_tp)
    t_dn = rem(t + n_tp - 1, n_tp)
    t_far = rem(t + 2, n_tp)
    x_up = rem(x + 1, n_chip)
    x_dn = rem(x + n_chip - 1, n_chip)
    x_far = rem(x + 2, n_chip)
    up_ep = x_up * 2 + c
    dn_ep = x_dn * 2 + c
    mate_ep = x * 2 + (1 - c)

    def block(ep, tp):
        return ep * n_tp + tp

    own = block(e, t)
    own_copies = [
        pltpu.make_async_copy(tokens, tok.at[own, pl.ds(0, n_tok)], load_sem.at[0]),
        pltpu.make_async_copy(id_rows, tok.at[own, pl.ds(n_tok, ID_ROWS)], load_sem.at[1]),
    ]
    for copy in own_copies:
        copy.start()
    w_copies = []
    for i in range(n_loc):
        w_copies.append(pltpu.make_async_copy(w_up.at[i], up.at[i], w_sem.at[0, i]))
        w_copies.append(pltpu.make_async_copy(w_down.at[i], down.at[i], w_sem.at[1, i]))
    for copy in w_copies:
        copy.start()

    barrier = pltpu.get_barrier_semaphore()
    for tp in (t_up, t_dn):
        pl.semaphore_signal(barrier, inc=1, device_id={"tp": tp, "ep": e}, device_id_type=MESH)
    for step in range(1, n_ep):
        pl.semaphore_signal(barrier, inc=1, device_id={"tp": t, "ep": rem(e + step, n_ep)}, device_id_type=MESH)

    row_i = lax.broadcasted_iota(jnp.int32, (n_tok, n_tok), 0)
    col_i = lax.broadcasted_iota(jnp.int32, (n_tok, n_tok), 1)
    tri[...] = jnp.where(row_i < col_i, 1.0, 0.0).astype(jnp.bfloat16)
    lower = jnp.where(row_i > col_i, 1.0, 0.0).astype(jnp.bfloat16)
    lanes = max(128, n_exp)
    lane_i = lax.broadcasted_iota(jnp.int32, (n_tok, lanes), 1)
    hit_sum = jnp.zeros((n_tok, lanes), jnp.float32)
    for j in range(n_top):
        hit_sum = hit_sum + jnp.where(ids_col[:, j:j + 1] == lane_i, 1.0, 0.0)
    prior = jnp.dot(lower, hit_sum.astype(jnp.bfloat16), preferred_element_type=jnp.float32)
    for j in range(n_top):
        ids_j = ids_col[:, j:j + 1]
        rank = jnp.sum(jnp.where(ids_j == lane_i, prior, 0.0), axis=1, keepdims=True).astype(jnp.int32)
        slot_col[:, j:j + 1] = jnp.where(rank < slot_cap, ids_j * slot_cap + rank, -1)
    acc[...] = jnp.zeros_like(acc)

    sends = []

    def send(make):
        make().start()
        sends.append(make)

    def remote(src, dst, send_sem, recv_sem, tp, ep):
        return pltpu.make_async_remote_copy(src_ref=src, dst_ref=dst, send_sem=send_sem, recv_sem=recv_sem,
                                            device_id={"tp": tp, "ep": ep}, device_id_type=MESH)

    n_full = [0]
    n_half = [0]

    def send_full(src, tp, ep):
        n = n_full[0]
        n_full[0] += 1

        def make():
            b = block(*src)
            return remote(tok.at[b], tok.at[b], full_send.at[n], full_recv.at[b], tp, ep)
        send(make)

    def half_of(b, which):
        return tok.at[b, pl.ds(0, half_rows)] if which == 0 else tok.at[b, pl.ds(half_rows, rows - half_rows)]

    def send_half(src, which, tp, ep):
        n = n_half[0]
        n_half[0] += 1

        def make():
            b = block(*src)
            ref = half_of(b, which)
            return remote(ref, ref, half_send.at[n], half_recv.at[which, b], tp, ep)
        send(make)

    def wait_full(src):
        b = block(*src)
        pltpu.make_async_copy(tok.at[b], tok.at[b], full_recv.at[b]).wait()

    def wait_half(src, which):
        b = block(*src)
        ref = half_of(b, which)
        pltpu.make_async_copy(ref, ref, half_recv.at[which, b]).wait()

    def spread(src):
        send_full(src, t, up_ep)
        send_full(src, t, dn_ep)
        send_full(src, t, mate_ep)

    for copy in own_copies:
        copy.wait()
    pl.semaphore_wait(barrier, n_ep + 1)
    send_full((e, t), t_up, e)
    send_full((e, t), t_dn, e)
    spread((e, t))
    wait_full((e, t_dn))
    send_half((e, t_dn), 0, t_up, e)
    spread((e, t_dn))
    wait_full((e, t_up))
    send_half((e, t_up), 1, t_dn, e)
    spread((e, t_up))
    wait_half((e, t_far), 0)
    wait_half((e, t_far), 1)
    spread((e, t_far))

    def relay(tp):
        wait_full((dn_ep, tp))
        send_half((dn_ep, tp), 0, t, up_ep)
        send_full((dn_ep, tp), t, mate_ep)
        wait_full((up_ep, tp))
        send_half((up_ep, tp), 1, t, dn_ep)
        send_full((up_ep, tp), t, mate_ep)

    far_ep = x_far * 2 + c

    def far_block(tp):
        wait_half((far_ep, tp), 0)
        wait_half((far_ep, tp), 1)
        send_full((far_ep, tp), t, mate_ep)

    def source_ep(k):
        return rem(x + div(k, 2), n_chip) * 2 + rem(c + k, 2)

    def pick(s):
        exp_i = lax.broadcasted_iota(jnp.int32, (n_loc, n_tok), 0) + e * n_loc
        hits = []
        for tp in range(n_tp):
            row = tok[block(s, tp), n_tok:rows, 0:n_top * n_tok].astype(jnp.float32)
            hit = jnp.zeros((n_loc, n_tok), jnp.float32)
            for j in range(n_top):
                ids = row[0:1, j * n_tok:(j + 1) * n_tok].astype(jnp.int32)
                hit = hit + jnp.where(ids == exp_i, 1.0, 0.0)
            hits.append(hit)
        hit = jnp.concatenate(hits, axis=0)
        prior = jnp.dot(hit.astype(jnp.bfloat16), tri[...], preferred_element_type=jnp.float32)
        rank = jnp.where(hit > 0.0, prior, -1.0)
        slot_i = lax.broadcasted_iota(jnp.int32, (slot_cap, n_tok), 0).astype(jnp.float32)
        for tp in range(n_tp):
            picks = []
            for i in range(n_loc):
                r = tp * n_loc + i
                picks.append(jnp.where(rank[r:r + 1] == slot_i, 1.0, 0.0))
            onehot = jnp.concatenate(picks, axis=0).astype(jnp.bfloat16)
            got = jnp.dot(onehot, tok[block(s, tp), 0:n_tok, :], preferred_element_type=jnp.float32)
            got = got.astype(jnp.bfloat16)
            for i in range(n_loc):
                xbuf[i, tp * slot_cap:(tp + 1) * slot_cap, :] = got[i * slot_cap:(i + 1) * slot_cap]

    def ffn(i):
        h = rem(i, 2)

        def one(q, carry):
            w = h * half_exp + q
            pre = jnp.dot(xbuf[w], up[w], preferred_element_type=jnp.float32)
            act = jax.nn.gelu(pre, approximate=True).astype(jnp.bfloat16)
            res = jnp.dot(act, down[w], preferred_element_type=jnp.float32)
            for tp in range(n_tp):
                part[i, tp, pl.ds(pl.multiple_of(q * slot_cap, slot_cap), slot_cap), :] = (
                    res[tp * slot_cap:(tp + 1) * slot_cap])
            return carry

        lax.fori_loop(0, half_exp, one, 0)

    lo = pl.ds(0, sub_half)
    hi = pl.ds(sub_half, sub_half)

    def r_copy(src, dst, send_sem, recv_sem, tp):
        return pltpu.make_async_remote_copy(src_ref=src, dst_ref=dst, send_sem=send_sem, recv_sem=recv_sem,
                                            device_id={"tp": tp, "ep": e}, device_id_type=MESH)

    def first_copies(i):
        return [
            r_copy(part.at[i, t_far, lo], r1.at[0, i], r1_send.at[0, i], r1_recv.at[0, i], t_up),
            r_copy(part.at[i, t_far, hi], r1.at[1, i], r1_send.at[1, i], r1_recv.at[1, i], t_dn),
            r_copy(part.at[i, t_up, hi], r2.at[0, i, hi], r2_send.at[0, 1, i], r2_recv.at[0, 1, i], t_up),
            r_copy(part.at[i, t_dn, lo], r2.at[1, i, lo], r2_send.at[1, 0, i], r2_recv.at[1, 0, i], t_dn),
        ]

    def second_copies(i):
        return [
            r_copy(part.at[i, t_up, lo], r2.at[0, i, lo], r2_send.at[0, 0, i], r2_recv.at[0, 0, i], t_up),
            r_copy(part.at[i, t_dn, hi], r2.at[1, i, hi], r2_send.at[1, 1, i], r2_recv.at[1, 1, i], t_dn),
        ]

    def back_copy(i):
        return pltpu.make_async_remote_copy(
            src_ref=red.at[i], dst_ref=ret.at[e, rem(i, 2)], send_sem=ret_send.at[i], recv_sem=ret_recv.at[i],
            device_id={"tp": t, "ep": source_ep(div(i, 2))}, device_id_type=MESH)

    def relay_sums(i):
        first = first_copies(i)
        first[0].wait_recv()
        part[i, t_up, lo, :] = part[i, t_up, lo, :] + r1[0, i]
        second = second_copies(i)
        second[0].start()
        first[1].wait_recv()
        part[i, t_dn, hi, :] = part[i, t_dn, hi, :] + r1[1, i]
        second[1].start()

    def finish(i):
        first = first_copies(i)
        second = second_copies(i)
        first[2].wait_recv()
        first[3].wait_recv()
        second[0].wait_recv()
        second[1].wait_recv()
        total = (part[i, t] + r2[0, i] + r2[1, i]).astype(jnp.bfloat16)

        @pl.when(i < 2)
        def _():
            ret[e, rem(i, 2)] = total

        @pl.when(i >= 2)
        def _():
            red[i] = total
            back_copy(i).start()

    def combine(i):
        k = div(i, 2)
        h = rem(i, 2)

        @pl.when(i >= 2)
        def _():
            back_copy(i).wait_recv()
        d = rem(x + n_chip - div(k, 2), n_chip) * 2 + rem(c + k, 2)
        base = (d * 2 + h) * sub_rows
        slot_i = lax.broadcasted_iota(jnp.int32, (n_tok, sub_rows), 1) + base
        rows_in = ret[d, h]
        add = jnp.zeros((n_tok, hidden), jnp.float32)
        for j in range(n_top):
            onehot = jnp.where(slot_col[:, j:j + 1] == slot_i, 1.0, 0.0).astype(jnp.bfloat16)
            add = add + gates[:, j:j + 1] * jnp.dot(onehot, rows_in, preferred_element_type=jnp.float32)
        acc[...] = acc[...] + add

    for copy in w_copies:
        copy.wait()

    def step(i, carry):
        @pl.when(i == 0)
        def _():
            relay(t)

        @pl.when(i == 1)
        def _():
            relay(t_dn)
            relay(t_up)

        @pl.when(i == 3)
        def _():
            relay(t_far)

        @pl.when(i == 8)
        def _():
            for tp in (t, t_dn, t_up, t_far):
                far_block(tp)

        for k in (1, 3, 5, 7):
            @pl.when(i == 2 * k)
            def _(k=k):
                for tp in range(n_tp):
                    wait_full((source_ep(k), tp))

        @pl.when(i < n_sub)
        def _():
            @pl.when(rem(i, 2) == 0)
            def _():
                pick(source_ep(div(i, 2)))
            ffn(i)
            for copy in first_copies(i):
                copy.start()

        @pl.when((i >= 1) & (i < n_sub + 1))
        def _():
            relay_sums(i - 1)

        @pl.when((i >= 2) & (i < n_sub + 2))
        def _():
            finish(i - 2)

        @pl.when(i >= 3)
        def _():
            combine(i - 3)
        return carry

    lax.fori_loop(0, n_sub + 3, step, 0)
    out[...] = acc[...].astype(out.dtype)

    for make in sends:
        make().wait_send()

    def drain(i, carry):
        for copy in first_copies(i) + second_copies(i):
            copy.wait_send()

        @pl.when(i >= 2)
        def _():
            back_copy(i).wait_send()
        return carry

    lax.fori_loop(0, n_sub, drain, 0)


def solution(mesh):
    n_tp, n_ep = mesh.shape["tp"], mesh.shape["ep"]
    row_spec = P(("dp", "ep", "tp"), None)

    def local_moe(tokens, expert_ids, gate_vals, w_up, w_down):
        n_tok, hidden = tokens.shape
        n_top = expert_ids.shape[1]
        n_loc, _, ffn_dim = w_up.shape
        n_exp = n_loc * n_ep
        slot_cap = capacity(n_tok, n_top, n_exp)
        id_row = jnp.zeros((ID_ROWS, hidden), jnp.bfloat16)
        flat = expert_ids.T.reshape(1, n_top * n_tok).astype(jnp.bfloat16)
        id_row = jnp.pad(flat, ((0, ID_ROWS - 1), (0, hidden - n_top * n_tok)))
        rows = n_tok + ID_ROWS
        n_src = n_ep * n_tp
        n_sub = 2 * n_ep
        sub_rows = n_loc // 2 * slot_cap
        any_spec = pl.BlockSpec(memory_space=pl.ANY)
        vmem_spec = pl.BlockSpec(memory_space=pltpu.VMEM)
        dma = pltpu.SemaphoreType.DMA
        return pl.pallas_call(
            functools.partial(moe_kernel, n_tp, n_ep, slot_cap),
            out_shape=jax.ShapeDtypeStruct((n_tok, hidden), jnp.bfloat16),
            in_specs=[any_spec, any_spec, vmem_spec, vmem_spec, any_spec, any_spec],
            out_specs=vmem_spec,
            scratch_shapes=[
                pltpu.VMEM((n_src, rows, hidden), jnp.bfloat16),
                pltpu.VMEM((n_loc, hidden, ffn_dim), jnp.bfloat16),
                pltpu.VMEM((n_loc, ffn_dim, hidden), jnp.bfloat16),
                pltpu.VMEM((n_tok, n_tok), jnp.bfloat16),
                pltpu.VMEM((n_loc, n_tp * slot_cap, hidden), jnp.bfloat16),
                pltpu.VMEM((n_sub, n_tp, sub_rows, hidden), jnp.float32),
                pltpu.VMEM((2, n_sub, sub_rows // 2, hidden), jnp.float32),
                pltpu.VMEM((2, n_sub, sub_rows, hidden), jnp.float32),
                pltpu.VMEM((n_sub, sub_rows, hidden), jnp.bfloat16),
                pltpu.VMEM((n_ep, 2, sub_rows, hidden), jnp.bfloat16),
                pltpu.VMEM((n_tok, n_top), jnp.int32),
                pltpu.VMEM((n_tok, hidden), jnp.float32),
                dma((2,)), dma((2, n_loc)),
                dma((n_src,)), dma((n_src,)), dma((n_src,)), dma((2, n_src)),
                dma((2, n_sub)), dma((2, n_sub)),
                dma((2, 2, n_sub)), dma((2, 2, n_sub)),
                dma((n_sub,)), dma((n_sub,)),
            ],
            compiler_params=pltpu.CompilerParams(
                collective_id=0, has_side_effects=True, vmem_limit_bytes=67043328),
        )(tokens, id_row, expert_ids, gate_vals, w_up, w_down)

    return jax.shard_map(local_moe, mesh=mesh,
                         in_specs=(row_spec, row_spec, row_spec, P("ep", None, "tp"), P("ep", "tp", None)),
                         out_specs=row_spec, check_vma=False)
```

```python
import functools

import jax
import jax.numpy as jnp
from jax import lax
from jax.experimental import pallas as pl
from jax.experimental.pallas import tpu as pltpu
from jax.sharding import PartitionSpec as P

MESH = pl.DeviceIdType.MESH
ID_ROWS = 16


def capacity(tok_count, n_top, n_exp):
    return ((5 * tok_count * n_top) // (4 * n_exp) + 7) // 8 * 8


def rem(a, b):
    return a % b if isinstance(a, int) else lax.rem(a, b)


def div(a, b):
    return a // b if isinstance(a, int) else lax.div(a, b)


def moe_kernel(n_tp, n_ep, slot_cap, tokens, ids_row, gates_row, w_up, w_down, out,
               tok, up, down, tri, xbuf, part, r1, r2, red, ret, slot_col, gates, acc,
               load_sem, w_sem, full_send, full_recv, half_send, half_recv,
               r1_send, r1_recv, r2_send, r2_recv, ret_send, ret_recv):
    t = lax.axis_index("tp")
    e = lax.axis_index("ep")
    n_chip = n_ep // 2
    x = div(e, 2)
    c = rem(e, 2)
    n_tok, hidden = tokens.shape
    n_loc = w_up.shape[0]
    n_top = ids_row.shape[0]
    n_exp = n_loc * n_ep
    rows = n_tok + ID_ROWS
    half_rows = n_tok // 2
    half_exp = n_loc // 2
    sub_rows = half_exp * slot_cap
    sub_half = sub_rows // 2
    n_sub = 2 * n_ep
    t_up = rem(t + 1, n_tp)
    t_dn = rem(t + n_tp - 1, n_tp)
    t_far = rem(t + 2, n_tp)
    x_up = rem(x + 1, n_chip)
    x_dn = rem(x + n_chip - 1, n_chip)
    x_far = rem(x + 2, n_chip)
    up_ep = x_up * 2 + c
    dn_ep = x_dn * 2 + c
    mate_ep = x * 2 + (1 - c)

    def block(ep, tp):
        return ep * n_tp + tp

    own = block(e, t)
    own_copy = pltpu.make_async_copy(tokens, tok.at[own, pl.ds(0, n_tok)], load_sem)
    own_copy.start()
    w_copies = []
    for i in range(n_loc):
        w_copies.append(pltpu.make_async_copy(w_up.at[i], up.at[i], w_sem.at[0, i]))
        w_copies.append(pltpu.make_async_copy(w_down.at[i], down.at[i], w_sem.at[1, i]))
    for copy in w_copies:
        copy.start()

    barrier = pltpu.get_barrier_semaphore()
    for tp in (t_up, t_dn):
        pl.semaphore_signal(barrier, inc=1, device_id={"tp": tp, "ep": e}, device_id_type=MESH)
    for step in range(1, n_ep):
        pl.semaphore_signal(barrier, inc=1, device_id={"tp": t, "ep": rem(e + step, n_ep)}, device_id_type=MESH)

    ids_f = ids_row[...].astype(jnp.float32)
    flat = [ids_f[j:j + 1] for j in range(n_top)] + [jnp.zeros((1, hidden - n_top * n_tok), jnp.float32)]
    flat = jnp.concatenate(flat, axis=1).astype(jnp.bfloat16)
    tok[own, n_tok:rows, :] = jnp.broadcast_to(flat, (ID_ROWS, hidden))
    both = jnp.concatenate([ids_f, gates_row[...], jnp.zeros((8 - 2 * n_top, n_tok), jnp.float32)], axis=0)
    both = jnp.transpose(both)
    gates[...] = both[:, n_top:2 * n_top]
    ids_col = both[:, 0:n_top].astype(jnp.int32)

    row_i = lax.broadcasted_iota(jnp.int32, (n_tok, n_tok), 0)
    col_i = lax.broadcasted_iota(jnp.int32, (n_tok, n_tok), 1)
    tri[...] = jnp.where(row_i < col_i, 1.0, 0.0).astype(jnp.bfloat16)
    lower = jnp.where(row_i > col_i, 1.0, 0.0).astype(jnp.bfloat16)
    lanes = max(128, n_exp)
    lane_i = lax.broadcasted_iota(jnp.int32, (n_tok, lanes), 1)
    hit_sum = jnp.zeros((n_tok, lanes), jnp.float32)
    for j in range(n_top):
        hit_sum = hit_sum + jnp.where(ids_col[:, j:j + 1] == lane_i, 1.0, 0.0)
    prior = jnp.dot(lower, hit_sum.astype(jnp.bfloat16), preferred_element_type=jnp.float32)
    for j in range(n_top):
        ids_j = ids_col[:, j:j + 1]
        rank = jnp.sum(jnp.where(ids_j == lane_i, prior, 0.0), axis=1, keepdims=True).astype(jnp.int32)
        slot_col[:, j:j + 1] = jnp.where(rank < slot_cap, ids_j * slot_cap + rank, -1)
    acc[...] = jnp.zeros_like(acc)

    sends = []

    def send(make):
        make().start()
        sends.append(make)

    def remote(src, dst, send_sem, recv_sem, tp, ep):
        return pltpu.make_async_remote_copy(src_ref=src, dst_ref=dst, send_sem=send_sem, recv_sem=recv_sem,
                                            device_id={"tp": tp, "ep": ep}, device_id_type=MESH)

    n_full = [0]
    n_half = [0]

    def send_full(src, tp, ep):
        n = n_full[0]
        n_full[0] += 1

        def make():
            b = block(*src)
            return remote(tok.at[b], tok.at[b], full_send.at[n], full_recv.at[b], tp, ep)
        send(make)

    def half_of(b, which):
        return tok.at[b, pl.ds(0, half_rows)] if which == 0 else tok.at[b, pl.ds(half_rows, rows - half_rows)]

    def send_half(src, which, tp, ep):
        n = n_half[0]
        n_half[0] += 1

        def make():
            b = block(*src)
            ref = half_of(b, which)
            return remote(ref, ref, half_send.at[n], half_recv.at[which, b], tp, ep)
        send(make)

    def wait_full(src):
        b = block(*src)
        pltpu.make_async_copy(tok.at[b], tok.at[b], full_recv.at[b]).wait()

    def wait_half(src, which):
        b = block(*src)
        ref = half_of(b, which)
        pltpu.make_async_copy(ref, ref, half_recv.at[which, b]).wait()

    def spread(src):
        send_full(src, t, up_ep)
        send_full(src, t, dn_ep)
        send_full(src, t, mate_ep)

    own_copy.wait()
    pl.semaphore_wait(barrier, n_ep + 1)
    send_full((e, t), t_up, e)
    send_full((e, t), t_dn, e)
    spread((e, t))
    wait_full((e, t_dn))
    send_half((e, t_dn), 0, t_up, e)
    spread((e, t_dn))
    wait_full((e, t_up))
    send_half((e, t_up), 1, t_dn, e)
    spread((e, t_up))
    wait_half((e, t_far), 0)
    wait_half((e, t_far), 1)
    spread((e, t_far))

    def relay(tp):
        wait_full((dn_ep, tp))
        send_half((dn_ep, tp), 0, t, up_ep)
        send_full((dn_ep, tp), t, mate_ep)
        wait_full((up_ep, tp))
        send_half((up_ep, tp), 1, t, dn_ep)
        send_full((up_ep, tp), t, mate_ep)

    far_ep = x_far * 2 + c

    def far_block(tp):
        wait_half((far_ep, tp), 0)
        wait_half((far_ep, tp), 1)
        send_full((far_ep, tp), t, mate_ep)

    def source_ep(k):
        return rem(x + div(k, 2), n_chip) * 2 + rem(c + k, 2)

    def pick(s):
        exp_i = lax.broadcasted_iota(jnp.int32, (n_loc, n_tok), 0) + e * n_loc
        hits = []
        for tp in range(n_tp):
            row = tok[block(s, tp), n_tok:rows, 0:n_top * n_tok].astype(jnp.float32)
            hit = jnp.zeros((n_loc, n_tok), jnp.float32)
            for j in range(n_top):
                ids = row[0:1, j * n_tok:(j + 1) * n_tok].astype(jnp.int32)
                hit = hit + jnp.where(ids == exp_i, 1.0, 0.0)
            hits.append(hit)
        hit = jnp.concatenate(hits, axis=0)
        prior = jnp.dot(hit.astype(jnp.bfloat16), tri[...], preferred_element_type=jnp.float32)
        rank = jnp.where(hit > 0.0, prior, -1.0)
        slot_i = lax.broadcasted_iota(jnp.int32, (slot_cap, n_tok), 0).astype(jnp.float32)
        for tp in range(n_tp):
            picks = []
            for i in range(n_loc):
                r = tp * n_loc + i
                picks.append(jnp.where(rank[r:r + 1] == slot_i, 1.0, 0.0))
            onehot = jnp.concatenate(picks, axis=0).astype(jnp.bfloat16)
            got = jnp.dot(onehot, tok[block(s, tp), 0:n_tok, :], preferred_element_type=jnp.float32)
            got = got.astype(jnp.bfloat16)
            for i in range(n_loc):
                xbuf[i, tp * slot_cap:(tp + 1) * slot_cap, :] = got[i * slot_cap:(i + 1) * slot_cap]

    def ffn(i):
        h = rem(i, 2)

        def one(q, carry):
            w = h * half_exp + q
            pre = jnp.dot(xbuf[w], up[w], preferred_element_type=jnp.float32)
            act = jax.nn.gelu(pre, approximate=True).astype(jnp.bfloat16)
            res = jnp.dot(act, down[w], preferred_element_type=jnp.float32)
            for tp in range(n_tp):
                part[i, tp, pl.ds(pl.multiple_of(q * slot_cap, slot_cap), slot_cap), :] = (
                    res[tp * slot_cap:(tp + 1) * slot_cap])
            return carry

        lax.fori_loop(0, half_exp, one, 0)

    lo = pl.ds(0, sub_half)
    hi = pl.ds(sub_half, sub_half)

    def r_copy(src, dst, send_sem, recv_sem, tp):
        return pltpu.make_async_remote_copy(src_ref=src, dst_ref=dst, send_sem=send_sem, recv_sem=recv_sem,
                                            device_id={"tp": tp, "ep": e}, device_id_type=MESH)

    def first_copies(i):
        return [
            r_copy(part.at[i, t_far, lo], r1.at[0, i], r1_send.at[0, i], r1_recv.at[0, i], t_up),
            r_copy(part.at[i, t_far, hi], r1.at[1, i], r1_send.at[1, i], r1_recv.at[1, i], t_dn),
            r_copy(part.at[i, t_up, hi], r2.at[0, i, hi], r2_send.at[0, 1, i], r2_recv.at[0, 1, i], t_up),
            r_copy(part.at[i, t_dn, lo], r2.at[1, i, lo], r2_send.at[1, 0, i], r2_recv.at[1, 0, i], t_dn),
        ]

    def second_copies(i):
        return [
            r_copy(part.at[i, t_up, lo], r2.at[0, i, lo], r2_send.at[0, 0, i], r2_recv.at[0, 0, i], t_up),
            r_copy(part.at[i, t_dn, hi], r2.at[1, i, hi], r2_send.at[1, 1, i], r2_recv.at[1, 1, i], t_dn),
        ]

    def back_copy(i):
        return pltpu.make_async_remote_copy(
            src_ref=red.at[i], dst_ref=ret.at[e, rem(i, 2)], send_sem=ret_send.at[i], recv_sem=ret_recv.at[i],
            device_id={"tp": t, "ep": source_ep(div(i, 2))}, device_id_type=MESH)

    def relay_sums(i):
        first = first_copies(i)
        first[0].wait_recv()
        part[i, t_up, lo, :] = part[i, t_up, lo, :] + r1[0, i]
        second = second_copies(i)
        second[0].start()
        first[1].wait_recv()
        part[i, t_dn, hi, :] = part[i, t_dn, hi, :] + r1[1, i]
        second[1].start()

    def finish(i):
        first = first_copies(i)
        second = second_copies(i)
        first[2].wait_recv()
        first[3].wait_recv()
        second[0].wait_recv()
        second[1].wait_recv()
        total = (part[i, t] + r2[0, i] + r2[1, i]).astype(jnp.bfloat16)

        @pl.when(i < 2)
        def _():
            ret[e, rem(i, 2)] = total

        @pl.when(i >= 2)
        def _():
            red[i] = total
            back_copy(i).start()

    def combine(i):
        k = div(i, 2)
        h = rem(i, 2)

        @pl.when(i >= 2)
        def _():
            back_copy(i).wait_recv()
        d = rem(x + n_chip - div(k, 2), n_chip) * 2 + rem(c + k, 2)
        base = (d * 2 + h) * sub_rows
        slot_i = lax.broadcasted_iota(jnp.int32, (n_tok, sub_rows), 1) + base
        rows_in = ret[d, h]
        add = jnp.zeros((n_tok, hidden), jnp.float32)
        for j in range(n_top):
            onehot = jnp.where(slot_col[:, j:j + 1] == slot_i, 1.0, 0.0).astype(jnp.bfloat16)
            add = add + gates[:, j:j + 1] * jnp.dot(onehot, rows_in, preferred_element_type=jnp.float32)
        acc[...] = acc[...] + add

    for copy in w_copies:
        copy.wait()

    def step(i, carry):
        @pl.when(i == 0)
        def _():
            relay(t)

        @pl.when(i == 1)
        def _():
            relay(t_dn)
            relay(t_up)

        @pl.when(i == 4)
        def _():
            relay(t_far)

        @pl.when(i == 8)
        def _():
            for tp in (t, t_dn, t_up, t_far):
                far_block(tp)

        for k in (1, 3, 5, 7):
            @pl.when(i == 2 * k)
            def _(k=k):
                for tp in range(n_tp):
                    wait_full((source_ep(k), tp))

        @pl.when(i < n_sub)
        def _():
            @pl.when(rem(i, 2) == 0)
            def _():
                pick(source_ep(div(i, 2)))
            ffn(i)
            for copy in first_copies(i):
                copy.start()

        @pl.when((i >= 1) & (i < n_sub + 1))
        def _():
            relay_sums(i - 1)

        @pl.when((i >= 3) & (i < n_sub + 3))
        def _():
            finish(i - 3)

        @pl.when(i >= 5)
        def _():
            combine(i - 5)
        return carry

    lax.fori_loop(0, n_sub + 5, step, 0)
    out[...] = acc[...].astype(out.dtype)

    for make in sends:
        make().wait_send()

    def drain(i, carry):
        for copy in first_copies(i) + second_copies(i):
            copy.wait_send()

        @pl.when(i >= 2)
        def _():
            back_copy(i).wait_send()
        return carry

    lax.fori_loop(0, n_sub, drain, 0)


def solution(mesh):
    n_tp, n_ep = mesh.shape["tp"], mesh.shape["ep"]
    row_spec = P(("dp", "ep", "tp"), None)

    def local_moe(tokens, expert_ids, gate_vals, w_up, w_down):
        n_tok, hidden = tokens.shape
        n_top = expert_ids.shape[1]
        n_loc, _, ffn_dim = w_up.shape
        n_exp = n_loc * n_ep
        slot_cap = capacity(n_tok, n_top, n_exp)
        rows = n_tok + ID_ROWS
        n_src = n_ep * n_tp
        n_sub = 2 * n_ep
        sub_rows = n_loc // 2 * slot_cap
        any_spec = pl.BlockSpec(memory_space=pl.ANY)
        vmem_spec = pl.BlockSpec(memory_space=pltpu.VMEM)
        dma = pltpu.SemaphoreType.DMA
        return pl.pallas_call(
            functools.partial(moe_kernel, n_tp, n_ep, slot_cap),
            out_shape=jax.ShapeDtypeStruct((n_tok, hidden), jnp.bfloat16),
            in_specs=[any_spec, vmem_spec, vmem_spec, any_spec, any_spec],
            out_specs=vmem_spec,
            scratch_shapes=[
                pltpu.VMEM((n_src, rows, hidden), jnp.bfloat16),
                pltpu.VMEM((n_loc, hidden, ffn_dim), jnp.bfloat16),
                pltpu.VMEM((n_loc, ffn_dim, hidden), jnp.bfloat16),
                pltpu.VMEM((n_tok, n_tok), jnp.bfloat16),
                pltpu.VMEM((n_loc, n_tp * slot_cap, hidden), jnp.bfloat16),
                pltpu.VMEM((n_sub, n_tp, sub_rows, hidden), jnp.float32),
                pltpu.VMEM((2, n_sub, sub_rows // 2, hidden), jnp.float32),
                pltpu.VMEM((2, n_sub, sub_rows, hidden), jnp.float32),
                pltpu.VMEM((n_sub, sub_rows, hidden), jnp.bfloat16),
                pltpu.VMEM((n_ep, 2, sub_rows, hidden), jnp.bfloat16),
                pltpu.VMEM((n_tok, n_top), jnp.int32),
                pltpu.VMEM((n_tok, n_top), jnp.float32),
                pltpu.VMEM((n_tok, hidden), jnp.float32),
                dma, dma((2, n_loc)),
                dma((n_src,)), dma((n_src,)), dma((n_src,)), dma((2, n_src)),
                dma((2, n_sub)), dma((2, n_sub)),
                dma((2, 2, n_sub)), dma((2, 2, n_sub)),
                dma((n_sub,)), dma((n_sub,)),
            ],
            compiler_params=pltpu.CompilerParams(
                collective_id=0, has_side_effects=True, vmem_limit_bytes=67043328),
        )(tokens, expert_ids.T, gate_vals.T, w_up, w_down)

    return jax.shard_map(local_moe, mesh=mesh,
                         in_specs=(row_spec, row_spec, row_spec, P("ep", None, "tp"), P("ep", "tp", None)),
                         out_specs=row_spec, check_vma=False)
```

```python
import functools

import jax
import jax.numpy as jnp
from jax import lax
from jax.experimental import pallas as pl
from jax.experimental.pallas import tpu as pltpu
from jax.sharding import PartitionSpec as P

MESH = pl.DeviceIdType.MESH
ID_ROWS = 16
SIXTEENTHS = (10, 11, 12, 14, 16)


def capacity(tok_count, n_top, n_exp):
    return ((5 * tok_count * n_top) // (4 * n_exp) + 7) // 8 * 8


def rem(a, b):
    return a % b if isinstance(a, int) else lax.rem(a, b)


def div(a, b):
    return a // b if isinstance(a, int) else lax.div(a, b)


def moe_kernel(n_tp, n_ep, slot_cap, n_row, tokens, ids_row, gates_row, w_up, w_down, out,
               tok, up, down, tri, xbuf, gbuf, wide, part, r1, r2, red, ret, slot_col, gates, acc,
               load_sem, w_sem, full_send, full_recv, half_send, half_recv,
               r1_send, r1_recv, r2_send, r2_recv, ret_send, ret_recv):
    t = lax.axis_index("tp")
    e = lax.axis_index("ep")
    n_chip = n_ep // 2
    x = div(e, 2)
    c = rem(e, 2)
    n_tok, hidden = tokens.shape
    n_loc = w_up.shape[0]
    n_top = ids_row.shape[0]
    n_exp = n_loc * n_ep
    rows = n_tok + ID_ROWS
    half_rows = n_tok // 2
    n_slot = n_loc * slot_cap
    spans = row_spans(n_row)
    t_up = rem(t + 1, n_tp)
    t_dn = rem(t + n_tp - 1, n_tp)
    t_far = rem(t + 2, n_tp)
    x_up = rem(x + 1, n_chip)
    x_dn = rem(x + n_chip - 1, n_chip)
    x_far = rem(x + 2, n_chip)
    up_ep = x_up * 2 + c
    dn_ep = x_dn * 2 + c
    mate_ep = x * 2 + (1 - c)

    def block(ep, tp):
        return ep * n_tp + tp

    own = block(e, t)
    own_copy = pltpu.make_async_copy(tokens, tok.at[own, pl.ds(0, n_tok)], load_sem)
    own_copy.start()
    w_copies = []
    for i in range(n_loc):
        w_copies.append(pltpu.make_async_copy(w_up.at[i], up.at[i], w_sem.at[0, i]))
        w_copies.append(pltpu.make_async_copy(w_down.at[i], down.at[i], w_sem.at[1, i]))
    for copy in w_copies:
        copy.start()

    barrier = pltpu.get_barrier_semaphore()
    for tp in (t_up, t_dn):
        pl.semaphore_signal(barrier, inc=1, device_id={"tp": tp, "ep": e}, device_id_type=MESH)
    for step in range(1, n_ep):
        pl.semaphore_signal(barrier, inc=1, device_id={"tp": t, "ep": rem(e + step, n_ep)}, device_id_type=MESH)

    ids_f = ids_row[...].astype(jnp.float32)
    flat = [ids_f[j:j + 1] for j in range(n_top)] + [jnp.zeros((1, hidden - n_top * n_tok), jnp.float32)]
    flat = jnp.concatenate(flat, axis=1).astype(jnp.bfloat16)
    tok[own, n_tok:rows, :] = jnp.broadcast_to(flat, (ID_ROWS, hidden))
    both = jnp.concatenate([ids_f, gates_row[...], jnp.zeros((8 - 2 * n_top, n_tok), jnp.float32)], axis=0)
    both = jnp.transpose(both)
    gates[...] = both[:, n_top:2 * n_top]
    ids_col = both[:, 0:n_top].astype(jnp.int32)

    row_i = lax.broadcasted_iota(jnp.int32, (n_tok, n_tok), 0)
    col_i = lax.broadcasted_iota(jnp.int32, (n_tok, n_tok), 1)
    tri[...] = jnp.where(row_i < col_i, 1.0, 0.0).astype(jnp.bfloat16)
    lower = jnp.where(row_i > col_i, 1.0, 0.0).astype(jnp.bfloat16)
    lanes = max(128, n_exp)
    lane_i = lax.broadcasted_iota(jnp.int32, (n_tok, lanes), 1)
    hit_sum = jnp.zeros((n_tok, lanes), jnp.float32)
    for j in range(n_top):
        hit_sum = hit_sum + jnp.where(ids_col[:, j:j + 1] == lane_i, 1.0, 0.0)
    prior = jnp.dot(lower, hit_sum.astype(jnp.bfloat16), preferred_element_type=jnp.float32)
    kept = jnp.minimum(jnp.sum(hit_sum, axis=0, keepdims=True), float(slot_cap))
    kept = jnp.broadcast_to(kept, (16, lanes)).astype(jnp.bfloat16)
    shift = n_loc.bit_length() - 1
    from_i = lax.broadcasted_iota(jnp.int32, (lanes, lanes), 0)
    to_i = lax.broadcasted_iota(jnp.int32, (lanes, lanes), 1)
    ahead = jnp.where((from_i < to_i) & ((from_i >> shift) == (to_i >> shift)), 1.0, 0.0).astype(jnp.bfloat16)
    offset = jnp.dot(kept, ahead, preferred_element_type=jnp.float32)[0:1]
    for j in range(n_top):
        ids_j = ids_col[:, j:j + 1]
        mine = ids_j == lane_i
        rank = jnp.sum(jnp.where(mine, prior, 0.0), axis=1, keepdims=True).astype(jnp.int32)
        place = jnp.sum(jnp.where(mine, prior + offset, 0.0), axis=1, keepdims=True).astype(jnp.int32)
        slot_col[:, j:j + 1] = jnp.where(rank < slot_cap, (ids_j >> shift) * n_row + place, -1)
    acc[...] = jnp.zeros_like(acc)

    sends = []

    def send(make):
        make().start()
        sends.append(make)

    def remote(src, dst, send_sem, recv_sem, tp, ep):
        return pltpu.make_async_remote_copy(src_ref=src, dst_ref=dst, send_sem=send_sem, recv_sem=recv_sem,
                                            device_id={"tp": tp, "ep": ep}, device_id_type=MESH)

    n_full = [0]
    n_half = [0]

    def send_full(src, tp, ep):
        n = n_full[0]
        n_full[0] += 1

        def make():
            b = block(*src)
            return remote(tok.at[b], tok.at[b], full_send.at[n], full_recv.at[b], tp, ep)
        send(make)

    def half_of(b, which):
        return tok.at[b, pl.ds(0, half_rows)] if which == 0 else tok.at[b, pl.ds(half_rows, rows - half_rows)]

    def send_half(src, which, tp, ep):
        n = n_half[0]
        n_half[0] += 1

        def make():
            b = block(*src)
            ref = half_of(b, which)
            return remote(ref, ref, half_send.at[n], half_recv.at[which, b], tp, ep)
        send(make)

    def wait_full(src):
        b = block(*src)
        pltpu.make_async_copy(tok.at[b], tok.at[b], full_recv.at[b]).wait()

    def wait_half(src, which):
        b = block(*src)
        ref = half_of(b, which)
        pltpu.make_async_copy(ref, ref, half_recv.at[which, b]).wait()

    def spread(src):
        send_full(src, t, up_ep)
        send_full(src, t, dn_ep)
        send_full(src, t, mate_ep)

    own_copy.wait()
    pl.semaphore_wait(barrier, n_ep + 1)
    send_full((e, t), t_up, e)
    send_full((e, t), t_dn, e)
    spread((e, t))
    wait_full((e, t_dn))
    send_half((e, t_dn), 0, t_up, e)
    spread((e, t_dn))
    wait_full((e, t_up))
    send_half((e, t_up), 1, t_dn, e)
    spread((e, t_up))
    wait_half((e, t_far), 0)
    wait_half((e, t_far), 1)
    spread((e, t_far))

    def relay(tp):
        wait_full((dn_ep, tp))
        send_half((dn_ep, tp), 0, t, up_ep)
        send_full((dn_ep, tp), t, mate_ep)
        wait_full((up_ep, tp))
        send_half((up_ep, tp), 1, t, dn_ep)
        send_full((up_ep, tp), t, mate_ep)

    far_ep = x_far * 2 + c

    def far_block(tp):
        wait_half((far_ep, tp), 0)
        wait_half((far_ep, tp), 1)
        send_full((far_ep, tp), t, mate_ep)

    def offsets(k):
        late = div(k, 4)
        dx = (1 - late) * div(k, 2) + late * (3 - rem(div(k - 3, 2), 2))
        dc = (1 - late) * rem(k, 2) + late * div(k - 4, 2)
        return dx, dc

    def source_ep(k):
        dx, dc = offsets(k)
        return rem(x + dx, n_chip) * 2 + rem(c + dc, 2)

    def pick(s):
        exp_i = lax.broadcasted_iota(jnp.int32, (n_loc, n_tok), 0) + e * n_loc
        hits = []
        for tp in range(n_tp):
            row = tok[block(s, tp), n_tok:rows, 0:n_top * n_tok].astype(jnp.float32)
            hit = jnp.zeros((n_loc, n_tok), jnp.float32)
            for j in range(n_top):
                ids = row[0:1, j * n_tok:(j + 1) * n_tok].astype(jnp.int32)
                hit = hit + jnp.where(ids == exp_i, 1.0, 0.0)
            hits.append(hit)
        hit = jnp.concatenate(hits, axis=0)
        prior = jnp.dot(hit.astype(jnp.bfloat16), tri[...], preferred_element_type=jnp.float32)
        rank = jnp.where(hit > 0.0, prior, -1.0)
        kept = jnp.minimum(jnp.sum(hit, axis=1, keepdims=True), float(slot_cap))
        lane = lax.broadcasted_iota(jnp.int32, (n_loc, n_slot), 1)
        first = lax.broadcasted_iota(jnp.int32, (n_loc, n_slot), 0) * slot_cap
        inside = (lane >= first) & (lane < first + slot_cap)
        past = lane >= first + slot_cap
        in_rank = jnp.sum(jnp.where(inside, lane - first, 0).astype(jnp.float32), axis=0, keepdims=True)
        row_i = lax.broadcasted_iota(jnp.int32, (n_row, n_slot), 0).astype(jnp.float32)
        slot_i = lax.broadcasted_iota(jnp.int32, (slot_cap, n_tok), 0).astype(jnp.float32)
        for tp in range(n_tp):
            kept_tp = kept[tp * n_loc:(tp + 1) * n_loc]
            count = jnp.sum(jnp.where(inside, kept_tp, 0.0), axis=0, keepdims=True)
            start = jnp.sum(jnp.where(past, kept_tp, 0.0), axis=0, keepdims=True)
            place = jnp.where(in_rank < count, start + in_rank, -1.0)
            gbuf[tp] = jnp.where(place == row_i, 1.0, 0.0).astype(jnp.bfloat16)
            picks = []
            for i in range(n_loc):
                r = tp * n_loc + i
                picks.append(jnp.where(rank[r:r + 1] == slot_i, 1.0, 0.0))
            onehot = jnp.concatenate(picks, axis=0).astype(jnp.bfloat16)
            got = jnp.dot(onehot, tok[block(s, tp), 0:n_tok, :], preferred_element_type=jnp.float32)
            got = got.astype(jnp.bfloat16)
            for i in range(n_loc):
                xbuf[i, tp * slot_cap:(tp + 1) * slot_cap, :] = got[i * slot_cap:(i + 1) * slot_cap]

    def ffn(k):
        def one(w, carry):
            pre = jnp.dot(xbuf[w], up[w], preferred_element_type=jnp.float32)
            act = jax.nn.gelu(pre, approximate=True).astype(jnp.bfloat16)
            res = jnp.dot(act, down[w], preferred_element_type=jnp.float32)
            for tp in range(n_tp):
                wide[tp, pl.ds(pl.multiple_of(w * slot_cap, slot_cap), slot_cap), :] = (
                    res[tp * slot_cap:(tp + 1) * slot_cap])
            return carry

        lax.fori_loop(0, n_loc, one, 0)

        def squeeze(tp, carry):
            rest = wide[tp] * 0.5
            got = jnp.zeros((n_row, hidden), jnp.float32)
            for _ in range(3):
                piece = rest.astype(jnp.bfloat16)
                rest = rest - piece.astype(jnp.float32)
                got = got + jnp.dot(gbuf[tp], piece, preferred_element_type=jnp.float32)
            part[k, tp] = got * 2.0
            return carry

        lax.fori_loop(0, n_tp, squeeze, 0)

    def r_copy(src, dst, send_sem, recv_sem, tp):
        return pltpu.make_async_remote_copy(src_ref=src, dst_ref=dst, send_sem=send_sem, recv_sem=recv_sem,
                                            device_id={"tp": tp, "ep": e}, device_id_type=MESH)

    def far_copies(k, s):
        lo, hi = spans[s]
        return [
            r_copy(part.at[k, t_far, lo], r1.at[k, lo], r1_send.at[0, s, k], r1_recv.at[0, s, k], t_up),
            r_copy(part.at[k, t_far, hi], r1.at[k, hi], r1_send.at[1, s, k], r1_recv.at[1, s, k], t_dn),
        ]

    def near_copies(k, s):
        lo, hi = spans[s]
        return [
            r_copy(part.at[k, t_up, hi], r2.at[0, k, hi], r2_send.at[0, 1, s, k], r2_recv.at[0, 1, s, k], t_up),
            r_copy(part.at[k, t_dn, lo], r2.at[1, k, lo], r2_send.at[1, 0, s, k], r2_recv.at[1, 0, s, k], t_dn),
        ]

    def sum_copies(k, s):
        lo, hi = spans[s]
        return [
            r_copy(part.at[k, t_up, lo], r2.at[0, k, lo], r2_send.at[0, 0, s, k], r2_recv.at[0, 0, s, k], t_up),
            r_copy(part.at[k, t_dn, hi], r2.at[1, k, hi], r2_send.at[1, 1, s, k], r2_recv.at[1, 1, s, k], t_dn),
        ]

    def back_copy(k):
        return pltpu.make_async_remote_copy(
            src_ref=red.at[k], dst_ref=ret.at[e], send_sem=ret_send.at[k], recv_sem=ret_recv.at[k],
            device_id={"tp": t, "ep": source_ep(k)}, device_id_type=MESH)

    def relay_sums(k):
        for s in range(len(spans)):
            lo, hi = spans[s]
            far = far_copies(k, s)
            total = sum_copies(k, s)
            far[0].wait_recv()
            part[k, t_up, lo, :] = part[k, t_up, lo, :] + r1[k, lo, :]
            total[0].start()
            far[1].wait_recv()
            part[k, t_dn, hi, :] = part[k, t_dn, hi, :] + r1[k, hi, :]
            total[1].start()

    def finish(k):
        for s in range(len(spans)):
            for copy in near_copies(k, s) + sum_copies(k, s):
                copy.wait_recv()
        total = (part[k, t] + r2[0, k] + r2[1, k]).astype(jnp.bfloat16)

        @pl.when(k == 0)
        def _():
            ret[e] = total

        @pl.when(k > 0)
        def _():
            red[k] = total
            back_copy(k).start()

    def combine(k):
        @pl.when(k > 0)
        def _():
            back_copy(k).wait_recv()
        dx, dc = offsets(k)
        d = rem(x + n_chip - dx, n_chip) * 2 + rem(c + dc, 2)
        row_i = lax.broadcasted_iota(jnp.int32, (n_tok, n_row), 1) + d * n_row
        rows_in = ret[d]
        add = jnp.zeros((n_tok, hidden), jnp.float32)
        for j in range(n_top):
            onehot = jnp.where(slot_col[:, j:j + 1] == row_i, 1.0, 0.0).astype(jnp.bfloat16)
            add = add + gates[:, j:j + 1] * jnp.dot(onehot, rows_in, preferred_element_type=jnp.float32)
        acc[...] = acc[...] + add

    for copy in w_copies:
        copy.wait()

    def step(k, carry):
        @pl.when(k == 0)
        def _():
            relay(t)

        @pl.when(k == 2)
        def _():
            relay(t_far)

        @pl.when(k == 5)
        def _():
            for tp in (t, t_dn, t_up, t_far):
                far_block(tp)

        for n in (1, 3, 6, 7):
            @pl.when(k == n)
            def _(n=n):
                for tp in range(n_tp):
                    wait_full((source_ep(n), tp))

        @pl.when(k < n_ep)
        def _():
            pick(source_ep(k))
            ffn(k)
            for s in range(len(spans)):
                for copy in far_copies(k, s):
                    copy.start()
            for s in range(len(spans)):
                for copy in near_copies(k, s):
                    copy.start()

        @pl.when((k >= 1) & (k < n_ep + 1))
        def _():
            relay_sums(k - 1)

        @pl.when(k == 1)
        def _():
            relay(t_dn)
            relay(t_up)

        @pl.when((k >= 3) & (k < n_ep + 3))
        def _():
            finish(k - 3)

        @pl.when(k >= 4)
        def _():
            combine(k - 4)
        return carry

    lax.fori_loop(0, n_ep + 4, step, 0)
    out[...] = acc[...].astype(out.dtype)

    for make in sends:
        make().wait_send()

    def drain(k, carry):
        for s in range(len(spans)):
            for copy in far_copies(k, s) + near_copies(k, s) + sum_copies(k, s):
                copy.wait_send()

        @pl.when(k > 0)
        def _():
            back_copy(k).wait_send()
        return carry

    lax.fori_loop(0, n_ep, drain, 0)


def most_kernel(n_tp, n_ep, slot_cap, sizes, ids_row, choice, stats, send_sem, recv_sem):
    t = lax.axis_index("tp")
    e = lax.axis_index("ep")
    n_top, n_tok = ids_row.shape
    n_dev = n_tp * n_ep
    me = e * n_tp + t

    def peer(step):
        other = rem(me + step, n_dev)
        return {"tp": rem(other, n_tp), "ep": div(other, n_tp)}

    barrier = pltpu.get_barrier_semaphore()

    def signal(step, carry):
        pl.semaphore_signal(barrier, inc=1, device_id=peer(step), device_id_type=MESH)
        return carry

    lax.fori_loop(1, n_dev, signal, 0)
    n_exp = sizes[-1] // slot_cap * n_ep
    exp_i = lax.broadcasted_iota(jnp.int32, (n_exp, n_tok), 0)
    hit = jnp.zeros((n_exp, n_tok), jnp.float32)
    for j in range(n_top):
        hit = hit + jnp.where(ids_row[j:j + 1] == exp_i, 1.0, 0.0)
    kept = jnp.minimum(jnp.sum(hit, axis=1, keepdims=True), float(slot_cap))
    n_loc = n_exp // n_ep
    loads = [jnp.sum(kept[g * n_loc:(g + 1) * n_loc], axis=0, keepdims=True) for g in range(n_ep)]
    load = functools.reduce(jnp.maximum, loads)
    stats[me] = jnp.broadcast_to(load, stats.shape[1:])
    pl.semaphore_wait(barrier, n_dev - 1)

    def copy(step):
        return pltpu.make_async_remote_copy(
            src_ref=stats.at[me], dst_ref=stats.at[me], send_sem=send_sem.at[step], recv_sem=recv_sem.at[step],
            device_id=peer(step), device_id_type=MESH)

    def start(step, carry):
        copy(step).start()
        return carry

    def wait(step, carry):
        copy(step).wait()
        return carry

    lax.fori_loop(1, n_dev, start, 0)
    lax.fori_loop(1, n_dev, wait, 0)
    most = jnp.max(stats[...])
    place = jnp.int32(0)
    for size in sizes[:-1]:
        place = place + jnp.where(most > float(size), 1, 0).astype(jnp.int32)
    choice[0] = place


def up8(n):
    return (n + 7) // 8 * 8


def row_spans(n_row):
    first = up8(n_row // 2)
    lo0 = up8(first // 2)
    hi1 = up8((n_row - first) // 2)
    mid = n_row - hi1
    return [(pl.ds(0, lo0), pl.ds(lo0, first - lo0)), (pl.ds(first, mid - first), pl.ds(mid, hi1))]


def solution(mesh):
    n_tp, n_ep = mesh.shape["tp"], mesh.shape["ep"]
    row_spec = P(("dp", "ep", "tp"), None)

    def local_moe(tokens, expert_ids, gate_vals, w_up, w_down):
        n_tok, hidden = tokens.shape
        n_top = expert_ids.shape[1]
        n_loc, _, ffn_dim = w_up.shape
        n_exp = n_loc * n_ep
        slot_cap = capacity(n_tok, n_top, n_exp)
        rows = n_tok + ID_ROWS
        n_src = n_ep * n_tp
        n_slot = n_loc * slot_cap
        any_spec = pl.BlockSpec(memory_space=pl.ANY)
        vmem_spec = pl.BlockSpec(memory_space=pltpu.VMEM)
        dma = pltpu.SemaphoreType.DMA
        sizes = sorted({up8(n_slot * part // 16) for part in SIXTEENTHS})
        ids_row, gates_row = expert_ids.T, gate_vals.T
        choice = pl.pallas_call(
            functools.partial(most_kernel, n_tp, n_ep, slot_cap, sizes),
            out_shape=jax.ShapeDtypeStruct((1,), jnp.int32),
            in_specs=[vmem_spec],
            out_specs=pl.BlockSpec(memory_space=pltpu.SMEM),
            scratch_shapes=[pltpu.VMEM((n_src, 1, 128), jnp.float32), dma((n_src,)), dma((n_src,))],
            compiler_params=pltpu.CompilerParams(collective_id=len(sizes), has_side_effects=True),
        )(ids_row)

        def moe(place):
            n_row = sizes[place]
            return pl.pallas_call(
                functools.partial(moe_kernel, n_tp, n_ep, slot_cap, n_row),
                out_shape=jax.ShapeDtypeStruct((n_tok, hidden), jnp.bfloat16),
                in_specs=[any_spec, vmem_spec, vmem_spec, any_spec, any_spec],
                out_specs=vmem_spec,
                scratch_shapes=[
                    pltpu.VMEM((n_src, rows, hidden), jnp.bfloat16),
                    pltpu.VMEM((n_loc, hidden, ffn_dim), jnp.bfloat16),
                    pltpu.VMEM((n_loc, ffn_dim, hidden), jnp.bfloat16),
                    pltpu.VMEM((n_tok, n_tok), jnp.bfloat16),
                    pltpu.VMEM((n_loc, n_tp * slot_cap, hidden), jnp.bfloat16),
                    pltpu.VMEM((n_tp, n_row, n_slot), jnp.bfloat16),
                    pltpu.VMEM((n_tp, n_slot, hidden), jnp.float32),
                    pltpu.VMEM((n_ep, n_tp, n_row, hidden), jnp.float32),
                    pltpu.VMEM((n_ep, n_row, hidden), jnp.float32),
                    pltpu.VMEM((2, n_ep, n_row, hidden), jnp.float32),
                    pltpu.VMEM((n_ep, n_row, hidden), jnp.bfloat16),
                    pltpu.VMEM((n_ep, n_row, hidden), jnp.bfloat16),
                    pltpu.VMEM((n_tok, n_top), jnp.int32),
                    pltpu.VMEM((n_tok, n_top), jnp.float32),
                    pltpu.VMEM((n_tok, hidden), jnp.float32),
                    dma, dma((2, n_loc)),
                    dma((n_src,)), dma((n_src,)), dma((n_src,)), dma((2, n_src)),
                    dma((2, 2, n_ep)), dma((2, 2, n_ep)),
                    dma((2, 2, 2, n_ep)), dma((2, 2, 2, n_ep)),
                    dma((n_ep,)), dma((n_ep,)),
                ],
                compiler_params=pltpu.CompilerParams(
                    collective_id=place, has_side_effects=True, vmem_limit_bytes=67043328),
            )(tokens, ids_row, gates_row, w_up, w_down)

        return lax.switch(choice[0], [functools.partial(moe, place) for place in range(len(sizes))])

    return jax.shard_map(local_moe, mesh=mesh,
                         in_specs=(row_spec, row_spec, row_spec, P("ep", None, "tp"), P("ep", "tp", None)),
                         out_specs=row_spec, check_vma=False)
```
